256 devices in a mesh: dp: 64 (over x, z, core), mp: 4 (over y).
Axes of the slice: x: 4, y: 4, z: 8, core: 2. Of those that a mesh axis runs over, the one named last changes fastest.
Arguments:
- features: bfloat16 [16384, 512], P('dp'), may hold values from -6 to 6
- adjacency: bfloat16 [4096, 4, 128, 128], P('dp'), may hold values from -0.125 to 0.125
- source_block: int32 [4096, 4], P('dp'), may hold values from 0 to 1
- edge_type: int32 [4096, 4], P('dp'), may hold values from 0 to 19
- target_block: int32 [4096, 4], P('dp'), may hold values from 0 to 1
- live_count: int32 [64, 64], P('dp'), may hold values from 3 to 4, as said below
- relation_weight: bfloat16 [20, 512, 512], P(None, None, 'mp'), may hold values from -0.25 to 0.25
- self_weight: bfloat16 [512, 512], P(None, 'mp'), may hold values from -0.25 to 0.25
- layer_bias: bfloat16 [512], P('mp'), may hold values from -3 to 3
- norm_gain: bfloat16 [512], replicated, may hold values from 0.5 to 1.5
Outputs:
- node_states: bfloat16 [16384, 512], P(('dp', 'mp'))
The draws below stay inside these ranges and needn't reach their ends.
Inputs may be any that keep to these rules, and one draw needn't show every extreme that they name: `source_block`: row s * 64 + d names a block among sender s's 2 blocks. `target_block`: row d * 64 + s names a block among receiver d's 2 blocks. live_count[d, s] live slots from sender s to receiver d, the first ones; some receiver has all 4 slots live from every sender.
All inputs are finite; a program needn't handle non-finite values.
Results may differ from the reference program's by a relative error of at most 0.007.
Values may be sent and summed in bfloat16 or wider, within the bound.
A program may use at most 128 MiB of HBM per device.

```python
import jax
import jax.numpy as jnp
from jax import lax

D = 512
R = 20
BLK = 128
NB_DEV = 2
IN_DEV = 256
PEERS = 64
SLOTS = 4
PAIRS = 4096
NODES = 16384


def draw_live_count(key, part):
    lowest = max(1, 3 * SLOTS // 4)
    drawn = jax.random.randint(jax.random.fold_in(key, 11), (PEERS, PEERS), lowest, SLOTS + 1)
    full_row = jax.random.randint(jax.random.fold_in(key, 12), (), 0, PEERS)
    row_index = jnp.arange(PEERS)[:, None]
    return jnp.where(row_index == full_row, SLOTS, drawn).astype(jnp.int32)


def with_ends(values, rng, smallest, largest):
    longest = values.shape.index(max(values.shape))
    spots = []
    for shift in (0, 1):
        where = [jax.random.randint(jax.random.fold_in(rng, axis), (), 0, length) for axis, length in enumerate(values.shape)]
        where[longest] = (where[longest] + shift) % values.shape[longest]
        spots.append(tuple(where))
    return values.at[spots[0]].set(smallest).at[spots[1]].set(largest)


def level_of(key, shape, shards, smallest, largest):
    def one(position, parts):
        draws = jax.random.uniform(jax.random.fold_in(jax.random.fold_in(key, 6), position), (parts,), jnp.float32, smallest / len(shards), largest / len(shards))
        return jnp.repeat(jnp.exp(draws), shape[position] // parts).reshape((-1,) + (1,) * (len(shape) - position - 1))

    factor_of = one(*shards[0])
    for cut in shards[1:]:
        factor_of = factor_of * one(*cut)
    return factor_of


def noise(rng, dims, deviation, limit, cuts=(), held_as=jnp.bfloat16):
    values = jax.random.normal(rng, dims, jnp.float32) * deviation
    if len(cuts) > 0:
        values = level_of(rng, dims, cuts, -0.22, 0.18) * values
    return jnp.clip(values, min=-limit, max=limit).astype(held_as)


def setup_inputs(seed: int = 0) -> dict:
    streams_of = jax.random.split(jax.random.key(seed), 11)
    features = noise(streams_of[0], (NODES, D), 1.0, 6.0, ((0, 64),))
    adjacency = noise(streams_of[1], (PAIRS, SLOTS, BLK, BLK), ((BLK * IN_DEV // NB_DEV) ** -0.5), 0.125, ((0, 64),))
    source_block = with_ends(jax.random.randint(streams_of[2], (PAIRS, SLOTS), 0, NB_DEV), jax.random.fold_in(streams_of[2], 1), 0, NB_DEV - 1).astype(jnp.int32)
    edge_type = with_ends(jax.random.randint(streams_of[3], (PAIRS, SLOTS), 0, R), jax.random.fold_in(streams_of[3], 1), 0, R - 1).astype(jnp.int32)
    target_block = with_ends(jax.random.randint(streams_of[4], (PAIRS, SLOTS), 0, NB_DEV), jax.random.fold_in(streams_of[4], 1), 0, NB_DEV - 1).astype(jnp.int32)
    live_count = draw_live_count(jax.random.fold_in(streams_of[10], 71), 0)
    relation_weight = noise(streams_of[6], (R, D, D), D ** -0.5, 0.25, ((2, 4),))
    self_weight = noise(streams_of[7], (D, D), D ** -0.5, 0.25, ((1, 4),))
    layer_bias = noise(streams_of[8], (D,), 0.5, 3.0, ((0, 4),))
    norm_gain = jnp.clip(1.0 + 0.1 * jax.random.normal(streams_of[9], (D,), jnp.float32), 0.5, 1.5).astype(jnp.bfloat16)
    return dict(features=features, adjacency=adjacency, source_block=source_block, edge_type=edge_type, target_block=target_block, live_count=live_count, relation_weight=relation_weight, self_weight=self_weight, layer_bias=layer_bias, norm_gain=norm_gain)


epsilon = 1e-05

def reference(features, adjacency, source_block, edge_type, target_block, live_count, relation_weight, self_weight, layer_bias, norm_gain):
    stacked = features.reshape(PEERS, NB_DEV, BLK, D)
    adj_tiles = adjacency.reshape(PEERS, PEERS * SLOTS, BLK, BLK)
    lookup_rows = (source_block * R + edge_type).reshape(PEERS, PEERS * SLOTS).astype(jnp.int32)
    active = jnp.arange(SLOTS, dtype=jnp.int32)[None, None, :] < live_count[:, :, None]
    matches = target_block.reshape(PEERS, PEERS, SLOTS)[:, :, :, None] == jnp.arange(NB_DEV, dtype=jnp.int32)[None, None, None, :]
    selector = jnp.logical_and(matches, active[:, :, :, None]).astype(jnp.float32)
    per_sender = jnp.transpose(selector, (1, 0, 2, 3))
    relations = relation_weight.astype(jnp.float32)

    def one_sender(running, inputs):
        block_rows, sender_tiles, sender_rows, sender_select = inputs
        lookup = jnp.einsum('bid,rdc->bric', block_rows.astype(jnp.float32), relations).astype(jnp.bfloat16)
        lookup = lookup.reshape(NB_DEV * R, BLK, D)
        chosen = jnp.take(lookup, sender_rows, axis=0)
        message = jnp.einsum('nij,njc->nic', sender_tiles.astype(jnp.float32), chosen.astype(jnp.float32))
        message = message.reshape(PEERS, SLOTS, BLK * D)
        summed = jnp.einsum('rkb,rkx->rbx', sender_select, message, precision=lax.Precision.HIGHEST)
        return (running + summed, None)
    initial = jnp.zeros((PEERS, NB_DEV, BLK * D), jnp.float32)
    running, ignored = lax.scan(one_sender, initial, (stacked, adj_tiles, lookup_rows, per_sender))
    aggregate = running.reshape(PEERS * NB_DEV * BLK, D)
    own_term = jnp.dot(features, self_weight, preferred_element_type=jnp.float32)
    hidden = jax.nn.relu(own_term + aggregate + layer_bias.astype(jnp.float32)).astype(jnp.bfloat16)
    values = lax.optimization_barrier(hidden).astype(jnp.float32)
    inverse_rms = lax.rsqrt(lax.optimization_barrier(jnp.mean(values * values, axis=1, keepdims=True)) + epsilon)
    return (values * inverse_rms * norm_gain.astype(jnp.float32)).astype(jnp.bfloat16)
```

```python
import functools

import jax
import jax.numpy as jnp
from jax import lax
from jax.experimental import pallas as pl
from jax.experimental.pallas import tpu as pltpu
from jax.sharding import PartitionSpec as P

BLK = 128
NX, NZ, NY = 4, 8, 4
GROUP = 2 * NX
PEERS = NX * NZ * 2
SLOTS = 4
BLOCKS = 2
ADJ_CHUNKS = 8
EPSILON = 1e-05
MESH = pl.DeviceIdType.MESH

X_FAR_PLUS = (4, 3, 2, 1)
Z_FAR_PLUS = (1,)
ROW_ORDER = (4, 3, 5, 2, 6, 1, 7, 0)


def pieces():
    table = {}
    for dz in range(NZ):
        plus = dz in X_FAR_PLUS
        far = ("xf", dz)
        table[far] = (2, dz, 0, (), "x+" if plus else "x-")
        table[("xp", dz)] = (1, dz, 0, (far,) if plus else (), "x+")
        table[("xm", dz)] = (3, dz, 0, () if plus else (far,), "x-")
    for dz, before, way in (
        (4, None, "z+"), (3, 4, "z+"), (2, 3, "z+"), (1, 2, "z+"), (5, None, "z-"), (6, 5, "z-"), (7, 6, "z-"),
    ):
        chain = () if before is None else (("az", before),)
        table[("az", dz)] = (0, dz, 0, (("xp", dz), ("xm", dz)) + chain, way)
    table[("fa",)] = (0, 0, 0, (("xp", 0), ("xm", 0), ("az", 1), ("az", 7)), None)
    for dx in range(NX):
        plus = dx in Z_FAR_PLUS
        far = ("bz", 4, dx)
        table[far] = (dx, 4, 1, (), "z+" if plus else "z-")
        table[("bz", 3, dx)] = (dx, 3, 1, (far,) if plus else (), "z+")
        table[("bz", 5, dx)] = (dx, 5, 1, () if plus else (far,), "z-")
        for dz, before, way in ((2, 3, "z+"), (1, 2, "z+"), (6, 5, "z-"), (7, 6, "z-")):
            table[("bz", dz, dx)] = (dx, dz, 1, (("bz", before, dx),), way)
    for dx, before, way in ((2, None, "x+"), (1, 2, "x+"), (3, None, "x-")):
        chain = () if before is None else (("bx", before),)
        table[("bx", dx)] = (dx, 0, 1, (("bz", 1, dx), ("bz", 7, dx)) + chain, way)
    table[("fb",)] = (0, 0, 1, (("bz", 1, 0), ("bz", 7, 0), ("bx", 1), ("bx", 3)), None)
    return table


ORDER = (
    ("bz", 4, 2), ("xf", 4), ("xm", 4), ("bz", 4, 1), ("bz", 4, 3), ("bz", 4, 0), ("xf", 3), ("bz", 3, 2),
    ("xm", 3), ("bz", 3, 3), ("bz", 3, 0), ("xf", 5), ("xp", 5), ("bz", 5, 1), ("xf", 2), ("xm", 2),
    ("xf", 6), ("xp", 6), ("xf", 1), ("xm", 1), ("xf", 7), ("xp", 7), ("xf", 0), ("xp", 0), ("bz", 5, 2),
    ("xp", 4), ("bz", 3, 1), ("bz", 5, 3), ("xp", 3), ("bz", 2, 2), ("bz", 5, 0), ("xm", 5), ("bz", 2, 3),
    ("bz", 6, 1), ("xp", 2), ("bz", 2, 0), ("xm", 6), ("bz", 6, 2), ("bz", 2, 1), ("xp", 1), ("bz", 6, 3),
    ("bz", 1, 2), ("xm", 7), ("bz", 6, 0), ("bz", 1, 3), ("xm", 0), ("bz", 7, 1), ("bz", 1, 0), ("az", 4),
    ("az", 5), ("bz", 7, 2), ("bz", 1, 1), ("bz", 7, 3), ("bz", 7, 0), ("az", 6), ("az", 3), ("bx", 2),
    ("bx", 3), ("az", 7), ("az", 2), ("bx", 1), ("az", 1), ("fb",), ("fa",),
)
PIECES = pieces()
SENT = tuple(name for name in PIECES if PIECES[name][4] is not None)
SLOT_OF = {name: n for n, name in enumerate(SENT)}


def layer_kernel(
    feat_in, adj_in, source_in, type_in, target_in, live_in, rel_in, self_in, bias_in, gain_in, out_ref,
    feat, adj, target, live, rel, self_w, bias, gain,
    table, msg, codes, by_group, group_got, by_z, z_got, weight,
    base, core_send, core_got, send_buf, got_buf, hidden, gathered,
    load_sem, adj_sem, send1, recv1, send2, recv2, core_s, core_r, piece_s, piece_r, mp_s, mp_r,
):
    me = lax.axis_index("dp")
    y = lax.axis_index("mp")
    c = me % 2
    z = (me // 2) % NZ
    x = me // (2 * NZ)
    p = x * 2 + c
    f32 = jnp.float32

    def dp_index(xi, zi, ci):
        return (xi * NZ + zi) * 2 + ci

    def at(dp, mp=None):
        return {"dp": dp, "mp": y if mp is None else mp}

    loads = [
        pltpu.make_async_copy(src, dst, load_sem.at[n])
        for n, (src, dst) in enumerate(
            ((target_in, target), (live_in, live), (feat_in, feat), (rel_in, rel),
             (self_in, self_w), (bias_in, bias), (gain_in, gain))
        )
    ]
    for load in loads[:4]:
        load.start()

    def adj_load(chunk):
        per = PEERS * SLOTS // ADJ_CHUNKS
        rows = pl.ds(chunk * per, per)
        return pltpu.make_async_copy(adj_in.at[rows], adj.at[rows], adj_sem.at[chunk])

    for chunk in range(ADJ_CHUNKS):
        adj_load(chunk).start()
    for load in loads[4:]:
        load.start()

    barrier = pltpu.get_barrier_semaphore()
    for j in range(1, GROUP):
        q = (p + j) % GROUP
        pl.semaphore_signal(barrier, inc=1, device_id=at(dp_index(q // 2, z, q % 2)), device_id_type=MESH)
    for j in range(1, NZ):
        pl.semaphore_signal(barrier, inc=1, device_id=at(dp_index(x, (z + j) % NZ, c)), device_id_type=MESH)
    for j in range(1, NY):
        pl.semaphore_signal(barrier, inc=1, device_id=at(me, (y + j) % NY), device_id_type=MESH)

    loads[0].wait()
    loads[1].wait()
    slot = lax.broadcasted_iota(jnp.int32, (SLOTS, PEERS), 0)
    codes[...] = jnp.zeros_like(codes)
    codes[0:SLOTS, 0:PEERS] = jnp.where(slot < live[...], target[...], BLOCKS)
    codes[...] = jnp.transpose(codes[...])
    for q in range(GROUP):
        by_group[q] = codes[pl.ds((q // 2) * 2 * NZ + q % 2, NZ, stride=2), :]

    loads[2].wait()
    loads[3].wait()
    relations = rel.shape[0]

    def table_step(i, carry):
        pair = jnp.concatenate([rel[2 * i], rel[2 * i + 1]], axis=1)
        got = jnp.dot(feat[...], pair, preferred_element_type=f32).astype(jnp.bfloat16)
        for b in range(BLOCKS):
            for h in range(2):
                table[b * relations + 2 * i + h] = got[b * BLK : (b + 1) * BLK, h * BLK : (h + 1) * BLK]
        return carry

    lax.fori_loop(0, relations // 2, table_step, 0, unroll=2)

    pl.semaphore_wait(barrier, GROUP - 1 + NZ - 1 + NY - 1)

    def group_copy(j):
        q = (p + j) % GROUP
        return pltpu.make_async_remote_copy(
            src_ref=by_group.at[q],
            dst_ref=group_got.at[pl.ds(pl.multiple_of(p * NZ, NZ), NZ)],
            send_sem=send1.at[j - 1],
            recv_sem=recv1.at[j - 1],
            device_id=at(dp_index(q // 2, z, q % 2)),
            device_id_type=MESH,
        )

    for j in range(1, GROUP):
        group_copy(j).start()
    group_got[pl.ds(pl.multiple_of(p * NZ, NZ), NZ), :] = by_group[p]

    def message_step(chunk, carry):
        adj_load(chunk).wait()
        per = PEERS // ADJ_CHUNKS
        step = 4

        def inner(i, carry):
            for u in range(step):
                d = chunk * per + i * step + u
                for k in range(SLOTS):
                    row = source_in[k, d] * relations + type_in[k, d]
                    n = d * SLOTS + k
                    msg[n] = jnp.dot(adj[n], table[row], preferred_element_type=f32)
            return carry

        return lax.fori_loop(0, per // step, inner, carry)

    lax.fori_loop(0, 4, message_step, 0)

    for j in range(1, GROUP):
        group_copy(j).wait_recv()
    for zi in range(NZ):
        by_z[zi] = group_got[pl.ds(zi, GROUP, stride=NZ), :]

    def z_copy(j):
        zi = (z + j) % NZ
        return pltpu.make_async_remote_copy(
            src_ref=by_z.at[zi],
            dst_ref=z_got.at[pl.ds(pl.multiple_of(z * GROUP, GROUP), GROUP)],
            send_sem=send2.at[j - 1],
            recv_sem=recv2.at[j - 1],
            device_id=at(dp_index(x, zi, c)),
            device_id_type=MESH,
        )

    for j in range(1, NZ):
        z_copy(j).start()
    z_got[pl.ds(pl.multiple_of(z * GROUP, GROUP), GROUP), :] = by_z[z]

    lax.fori_loop(4, ADJ_CHUNKS, message_step, 0)

    for load in loads[4:]:
        load.wait()
    base[...] = jnp.dot(feat[...], self_w[...], preferred_element_type=f32) + bias[...].astype(f32)

    for j in range(1, NZ):
        z_copy(j).wait_recv()
    routed = z_got[...]
    for k in range(SLOTS):
        column = jnp.broadcast_to(routed[:, k : k + 1], routed.shape)
        for b in range(BLOCKS):
            weight[k * BLOCKS + b] = (column == b).astype(f32)

    def own_sum(dx, dz, ci, b):
        xi = (x + dx) % NX
        zi = (z + dz) % NZ
        d = dp_index(xi, zi, ci)
        r = zi * GROUP + xi * 2 + ci
        total = None
        for k in range(SLOTS):
            term = msg[d * SLOTS + k] * weight[k * BLOCKS + b, pl.ds(r, 1), :]
            total = term if total is None else total + term
        return total

    other = 1 - c

    def core_copy(dz):
        return pltpu.make_async_remote_copy(
            src_ref=core_send.at[dz],
            dst_ref=core_got.at[dz],
            send_sem=core_s.at[dz],
            recv_sem=core_r.at[dz],
            device_id=at(dp_index(x, z, other)),
            device_id_type=MESH,
        )

    for dz in ROW_ORDER:

        def one(dx, carry, dz=dz):
            for b in range(BLOCKS):
                core_send[dz, dx, b] = own_sum(dx, dz, other, b).astype(jnp.bfloat16)
            return carry

        lax.fori_loop(0, NX, one, 0)
        core_copy(dz).start()

    def piece_copy(name):
        way = PIECES[name][4]
        to = {
            "x+": dp_index((x + 1) % NX, z, c),
            "x-": dp_index((x + NX - 1) % NX, z, c),
            "z+": dp_index(x, (z + 1) % NZ, c),
            "z-": dp_index(x, (z + NZ - 1) % NZ, c),
        }[way]
        n = SLOT_OF[name]
        return pltpu.make_async_remote_copy(
            src_ref=send_buf.at[n],
            dst_ref=got_buf.at[n],
            send_sem=piece_s.at[n],
            recv_sem=piece_r.at[n],
            device_id=at(to),
            device_id_type=MESH,
        )

    rows_in = set()
    pieces_in = set()
    for name in ORDER:
        dx, dz, b, adds, way = PIECES[name]
        if dz not in rows_in:
            core_copy(dz).wait_recv()
            rows_in.add(dz)
        for add in adds:
            if add not in pieces_in:
                piece_copy(add).wait_recv()
                pieces_in.add(add)
        total = own_sum(dx, dz, c, b) + core_got[dz, dx, b].astype(f32)
        for add in adds:
            total = total + got_buf[SLOT_OF[add]].astype(f32)
        if way is None:
            block = slice(b * BLK, (b + 1) * BLK)
            hidden[block, :] = jnp.maximum(base[block, :] + total, 0.0).astype(jnp.bfloat16)
        else:
            send_buf[SLOT_OF[name]] = total.astype(jnp.bfloat16)
            piece_copy(name).start()

    share = gathered.shape[1]

    def mp_copy(j):
        to = (y + j) % NY
        return pltpu.make_async_remote_copy(
            src_ref=hidden.at[pl.ds(pl.multiple_of(to * share, share), share)],
            dst_ref=gathered.at[y],
            send_sem=mp_s.at[j - 1],
            recv_sem=mp_r.at[j - 1],
            device_id=at(me, to),
            device_id_type=MESH,
        )

    for j in range(1, NY):
        mp_copy(j).start()
    gathered[y] = hidden[pl.ds(pl.multiple_of(y * share, share), share), :]
    for j in range(1, GROUP):
        group_copy(j).wait_send()
    for j in range(1, NZ):
        z_copy(j).wait_send()
    for dz in ROW_ORDER:
        core_copy(dz).wait_send()
    for name in SENT:
        piece_copy(name).wait_send()
    for j in range(1, NY):
        mp_copy(j).wait_recv()
    values = [gathered[i].astype(f32) for i in range(NY)]
    squares = sum(jnp.sum(v * v, axis=1, keepdims=True) for v in values)
    inverse = lax.rsqrt(squares / (NY * BLK) + EPSILON)
    for i, v in enumerate(values):
        cut = slice(i * BLK, (i + 1) * BLK)
        out_ref[:, cut] = (v * inverse * gain[i : i + 1, :].astype(f32)).astype(jnp.bfloat16)
    for j in range(1, NY):
        mp_copy(j).wait_send()


def per_device(
    features, adjacency, source_block, edge_type, target_block, live_count,
    relation_weight, self_weight, layer_bias, norm_gain,
):
    bf16, f32, i32 = jnp.bfloat16, jnp.float32, jnp.int32
    rows, width = features.shape
    relations = relation_weight.shape[0]
    slots = PEERS * SLOTS
    share = rows // NY
    dma = pltpu.SemaphoreType.DMA
    any_spec = pl.BlockSpec(memory_space=pl.ANY)
    smem_spec = pl.BlockSpec(memory_space=pltpu.SMEM)
    return pl.pallas_call(
        layer_kernel,
        name="layer",
        out_shape=jax.ShapeDtypeStruct((share, width), bf16),
        in_specs=[any_spec, any_spec, smem_spec, smem_spec] + [any_spec] * 6,
        out_specs=pl.BlockSpec(memory_space=pltpu.VMEM),
        scratch_shapes=[
            pltpu.VMEM((rows, width), bf16),
            pltpu.VMEM((slots, BLK, BLK), bf16),
            pltpu.VMEM((SLOTS, PEERS), i32),
            pltpu.VMEM((1, PEERS), i32),
            pltpu.VMEM((relations, width, BLK), bf16),
            pltpu.VMEM((width, BLK), bf16),
            pltpu.VMEM((1, BLK), bf16),
            pltpu.VMEM((NY, BLK), bf16),
            pltpu.VMEM((BLOCKS * relations, BLK, BLK), bf16),
            pltpu.VMEM((slots, BLK, BLK), f32),
            pltpu.VMEM((BLK, BLK), i32),
            pltpu.VMEM((GROUP, NZ, BLK), i32),
            pltpu.VMEM((PEERS, BLK), i32),
            pltpu.VMEM((NZ, GROUP, BLK), i32),
            pltpu.VMEM((PEERS, BLK), i32),
            pltpu.VMEM((SLOTS * BLOCKS, PEERS, BLK), f32),
            pltpu.VMEM((rows, BLK), f32),
            pltpu.VMEM((NZ, NX, BLOCKS, BLK, BLK), bf16),
            pltpu.VMEM((NZ, NX, BLOCKS, BLK, BLK), bf16),
            pltpu.VMEM((len(SENT), BLK, BLK), bf16),
            pltpu.VMEM((len(SENT), BLK, BLK), bf16),
            pltpu.VMEM((rows, BLK), bf16),
            pltpu.VMEM((NY, share, BLK), bf16),
            dma((7,)), dma((ADJ_CHUNKS,)),
            dma((GROUP - 1,)), dma((GROUP - 1,)), dma((NZ - 1,)), dma((NZ - 1,)),
            dma((NZ,)), dma((NZ,)), dma((len(SENT),)), dma((len(SENT),)), dma((NY - 1,)), dma((NY - 1,)),
        ],
        compiler_params=pltpu.CompilerParams(
            collective_id=0, has_side_effects=True, vmem_limit_bytes=60 * 1024 * 1024
        ),
    )(
        features, adjacency.reshape(slots, BLK, BLK), source_block.T, edge_type.T, target_block.T, live_count,
        relation_weight, self_weight, layer_bias.reshape(1, BLK), norm_gain.reshape(NY, BLK),
    )


def solution(mesh):
    return jax.shard_map(
        per_device,
        mesh=mesh,
        in_specs=(
            P("dp", None),
            P("dp", None, None, None),
            P("dp", None),
            P("dp", None),
            P("dp", None),
            P("dp", None),
            P(None, None, "mp"),
            P(None, "mp"),
            P("mp"),
            P(),
        ),
        out_specs=P(("dp", "mp"), None),
        check_vma=False,
    )
```
